1024 devices in a mesh: section: 32 (over y, x, core), expert: 32 (over z).
Axes of the slice: x: 4, y: 4, z: 32, core: 2. Of those that a mesh axis runs over, the one named last changes fastest.
Arguments:
- top_grad: bfloat16 [2, 512, 2048], P(None, 'expert'), may hold values from -6 to 6
- layer_input: bfloat16 [32, 2, 512, 2048], P('section', None, 'expert'), may hold values from -6 to 6
- expert_out: bfloat16 [32, 2, 512, 2, 2048], P('section', None, 'expert'), may hold values from -3 to 3
- router_w: float32 [32, 2048, 8], P('section'), may hold values from -0.375 to 0.375
- expert_ids: int32 [32, 2, 512, 2], P('section', None, 'expert'), may hold values from 0 to 7, as said below
- hidden: bfloat16 [32, 2, 256, 7168], P('section', None, None, 'expert'), may hold values from -0.59765625 to 0.59765625
- down_w: bfloat16 [32, 7168, 2048], P('section', 'expert'), may hold values from -0.0625 to 0.0625
Outputs:
- input_grad: bfloat16 [32, 2, 512, 2048], P('section', None, 'expert')
- router_grad: float32 [32, 2048, 8], P('section')
- hidden_grad: bfloat16 [32, 2, 256, 7168], P('section', None, None, 'expert')
- down_grad: bfloat16 [32, 7168, 2048], P('section', 'expert')
The draws below stay inside these ranges and needn't reach their ends.
Inputs may be any that keep to these rules, and one draw needn't show every extreme that they name: `expert_ids`: the two experts of a token differ. In each micro-batch, the 16 tokens of one device choose expert 0 at most 8 times, and exactly 8 times in some blocks of every draw.
All inputs are finite; a program needn't handle non-finite values.
Results may differ from the reference program's by a relative error of at most 0.024.
Values may be sent and summed in bfloat16 or wider, within the bound.
No kernel may reach another device: no remote copies, remote signals or barrier semaphores. Data moves between devices by JAX's collectives and lax.ppermute only.
A program may use at most 32 MiB of HBM per device.

```python
import jax
import jax.numpy as jnp
from jax import lax

D = 2048
FF = 7168
EXPERTS = 8
TOP = 2
MB = 2
TOK_MB = 16
CAP = 8
LAYERS = 32
TOKENS = 512
SLOTS = 256
N_EXPERT = 32


def draw_expert_ids(key, part):
    blocks = LAYERS * MB * (TOKENS // TOK_MB)
    key_count, key_order, key_first, key_step, key_flip = jax.random.split(key, 5)
    lowest = max(1, CAP // 4)
    counts = jax.random.randint(key_count, (blocks,), lowest, CAP + 1)
    counts = jnp.where(jnp.arange(blocks) % 3 == 0, CAP, counts)
    scores = jax.random.randint(key_order, (blocks, TOK_MB), 0, 1 << 20)
    scores = scores * TOK_MB + jnp.arange(TOK_MB, dtype=jnp.int32)[None, :]
    order = jnp.argsort(scores, axis=1)
    ranking = jnp.argsort(order, axis=1)
    chosen_zero = ranking < counts[:, None]
    other_a = jax.random.randint(key_first, (blocks, TOK_MB), 1, EXPERTS)
    offset_b = jax.random.randint(key_step, (blocks, TOK_MB), 1, EXPERTS - 1)
    other_b = 1 + (other_a - 1 + offset_b) % (EXPERTS - 1)
    first_id = jnp.where(chosen_zero, 0, other_a)
    second_id = jnp.where(chosen_zero, other_a, other_b)
    flipped = jax.random.randint(key_flip, (blocks, TOK_MB), 0, 2) == 1
    id_one = jnp.where(flipped, second_id, first_id)
    id_two = jnp.where(flipped, first_id, second_id)
    stacked = jnp.stack([id_one, id_two], axis=-1).astype(jnp.int32)
    return stacked.reshape(LAYERS, MB, TOKENS, TOP)


def block_scale(rng, shape, cuts, low, top_value):
    level, own = 1.0, jax.random.fold_in(rng, 6)
    for position, shards_of in cuts:
        steps = jnp.exp(jax.random.uniform(jax.random.fold_in(own, position), (shards_of,), jnp.float32, low / len(cuts), top_value / len(cuts)))
        level = level * jnp.repeat(steps, shape[position] // shards_of).reshape([-1 if axis == position else 1 for axis in range(len(shape))])
    return level


def normal_values(key, extent, scale, limit, cuts=(), kind=jnp.bfloat16):
    array = jax.random.normal(key, extent, jnp.float32) * scale
    if len(cuts) > 0:
        array = block_scale(key, extent, cuts, -0.22, 0.18) * array
    return jnp.clip(array, min=-limit, max=limit).astype(kind)


def setup_inputs(seed: int = 0) -> dict:
    keys = jax.random.split(jax.random.key(seed), 8)
    return {
        "top_grad": normal_values(keys[0], (MB, TOKENS, D), 1.0, 6.0, ((1, 32),)),
        "layer_input": normal_values(keys[1], (LAYERS, MB, TOKENS, D), 1.0, 6.0, ((0, 32), (2, 32))),
        "expert_out": normal_values(keys[2], (LAYERS, MB, TOKENS, TOP, D), 0.5, 3.0, ((0, 32), (2, 32))),
        "router_w": normal_values(keys[3], (LAYERS, D, EXPERTS), (D // 8) ** -0.5, 0.375, ((0, 32),), jnp.float32),
        "expert_ids": draw_expert_ids(jax.random.fold_in(keys[7], 71), 0),
        "hidden": normal_values(keys[5], (LAYERS, MB, SLOTS, FF), 0.1, 0.59765625, ((0, 32), (3, 32))),
        "down_w": normal_values(keys[6], (LAYERS, FF, D), FF ** -0.5, 0.0625, ((0, 32), (1, 32))),
    }


def gate_pair(inputs, weights, chosen):
    logits = jnp.einsum('mtd,de->mte', inputs.astype(jnp.float32), weights, precision=lax.Precision.HIGHEST)
    select = (chosen[..., None] == jnp.arange(weights.shape[1], dtype=jnp.int32)).astype(jnp.float32)
    picked = jnp.sum(select * logits[..., None, :], axis=-1)
    gate_first = jax.nn.sigmoid(picked[..., 0] - picked[..., 1])
    return gate_first, select


def backprop(cotangent, inputs, outputs, weights, select, gate_first):
    cot_float = cotangent.astype(jnp.float32)
    gate_dot = jnp.einsum('mtkd,mtd->mtk', outputs, cotangent, preferred_element_type=jnp.float32)
    logit_diff = gate_first * (1.0 - gate_first) * (gate_dot[..., 0] - gate_dot[..., 1])
    logit_grad = logit_diff[..., None] * (select[..., 0, :] - select[..., 1, :])
    passed = cot_float + jnp.einsum('mte,de->mtd', logit_grad, weights, precision=lax.Precision.HIGHEST)
    router_part = jnp.einsum('mtd,mte->de', inputs.astype(jnp.float32), logit_grad, precision=lax.Precision.HIGHEST)
    return passed.astype(jnp.bfloat16), router_part


def dispatch_rows(cotangent, gate_first, chosen, capacity):
    is_zero = (chosen == 0).astype(jnp.float32)
    zero_gate = gate_first * is_zero[..., 0] + (1.0 - gate_first) * is_zero[..., 1]
    routed = is_zero[..., 0] + is_zero[..., 1]
    slot_pos = (jnp.cumsum(routed, axis=-1) - routed).astype(jnp.int32)
    slot_ids = jnp.arange(capacity, dtype=jnp.int32)
    pick_table = ((slot_pos[..., None, :] == slot_ids[:, None]) & (routed[..., None, :] > 0.5)).astype(jnp.float32)
    scaled = zero_gate[..., None] * cotangent.astype(jnp.float32)
    rows_out = jnp.einsum('mbcu,mbud->mbcd', pick_table, scaled, precision=lax.Precision.HIGHEST)
    return rows_out.astype(jnp.bfloat16)


def expert_grads(section_parts):
    rows_out, saved_hidden, weight = section_parts
    flat_rows = rows_out.reshape(-1, rows_out.shape[-1])
    hidden_grad = lax.dot_general(flat_rows, weight, (((1,), (1,)), ((), ())), preferred_element_type=jnp.float32)
    hidden_grad = hidden_grad.astype(jnp.bfloat16).reshape(saved_hidden.shape)
    flat_hidden = saved_hidden.reshape(-1, saved_hidden.shape[-1])
    down_grad = lax.dot_general(flat_hidden, flat_rows, (((0,), (0,)), ((), ())), preferred_element_type=jnp.float32)
    return hidden_grad, down_grad.astype(jnp.bfloat16)


def reference(top_grad, layer_input, expert_out, router_w, expert_ids, hidden, down_w):
    def descend(cotangent, section_parts):
        inputs, outputs, weights, chosen = section_parts
        gate_first, select = gate_pair(inputs, weights, chosen)
        passed, router_part = backprop(cotangent, inputs, outputs, weights, select, gate_first)
        return passed, (passed, router_part / (MB * TOKENS), cotangent, gate_first)

    _, (input_grad, router_grad, section_dy, gate_all) = lax.scan(
        descend, top_grad, (layer_input, expert_out, router_w, expert_ids), reverse=True)

    def make_rows(section_parts):
        cotangent, gate_first, chosen = section_parts
        rows_out = dispatch_rows(cotangent.reshape(MB, N_EXPERT, TOK_MB, D),
                                 gate_first.reshape(MB, N_EXPERT, TOK_MB),
                                 chosen.reshape(MB, N_EXPERT, TOK_MB, TOP), CAP)
        return rows_out.reshape(MB, N_EXPERT * CAP, D)

    rows_all = lax.map(make_rows, (section_dy, gate_all, expert_ids))
    hidden_grad, down_grad = lax.map(expert_grads, (rows_all, hidden, down_w))
    return input_grad, router_grad, hidden_grad, down_grad
```

```python
import jax
import jax.numpy as jnp
from jax import lax
from jax.experimental import pallas as pl
from jax.experimental.pallas import tpu as pltpu
from jax.sharding import PartitionSpec as P

HIGH = lax.Precision.HIGHEST


def cascade_kernel(ur_ref, top_ref, out_ref):
    count = ur_ref.shape[0]
    cot = top_ref[0].astype(jnp.float32)
    for layer in reversed(range(count)):
        out_ref[layer] = cot.astype(jnp.bfloat16)
        if layer:
            prod = ur_ref[layer, 0].astype(jnp.float32) * cot
            half = prod[:, :128] + prod[:, 128:]
            diff = jnp.sum(jnp.sum(half, axis=1, keepdims=True), axis=0, keepdims=True)
            cot = cot + diff * ur_ref[layer, 1].astype(jnp.float32)
            cot = cot.astype(jnp.bfloat16).astype(jnp.float32)


def cascade(pairs, top_token):
    count = pairs.shape[0]
    return pl.pallas_call(
        cascade_kernel,
        out_shape=jax.ShapeDtypeStruct((count, 8, 256), jnp.bfloat16),
        name="cascade",
    )(pairs, top_token)


def swap(value):
    return lax.all_to_all(value, "section", 0, 0, tiled=True)


def to_half(value):
    peak = jnp.max(jnp.abs(value), axis=-1, keepdims=True)
    power = jnp.clip(jnp.ceil(jnp.log2(jnp.maximum(peak, 1e-30))), -100.0, 120.0)
    return (value * jnp.exp2(-power)).astype(jnp.float16), power[..., 0]


def per_device(top_grad, layer_input, expert_out, router_w, expert_ids, hidden, down_w):
    micro, tok, width = top_grad.shape
    tokens = micro * tok
    sections = lax.axis_size("section")
    groups = lax.axis_size("expert")
    capacity = tok // 2
    inputs = layer_input[0].reshape(tokens, width).astype(jnp.float32)
    outputs = expert_out[0].reshape(tokens, 2, width)
    router = router_w[0]
    experts = router.shape[1]
    chosen = expert_ids[0].reshape(tokens, 2)

    logits = jnp.dot(inputs, router, precision=HIGH)
    select = (chosen[..., None] == jnp.arange(experts, dtype=jnp.int32)).astype(jnp.float32)
    sign = select[:, 0] - select[:, 1]
    gate = jax.nn.sigmoid(jnp.sum(sign * logits, axis=-1))
    slope = gate * (1.0 - gate)
    out_diff = outputs[:, 0].astype(jnp.float32) - outputs[:, 1].astype(jnp.float32)
    step = lax.dot_general(sign, router, (((1,), (1,)), ((), ())), precision=HIGH)

    pairs = jnp.stack(
        [(slope[:, None] * out_diff).astype(jnp.bfloat16), step.astype(jnp.bfloat16)], axis=1
    ).reshape(tokens, 2, 8, width // 8)
    mine = lax.axis_index("section")
    top_token = lax.dynamic_slice_in_dim(top_grad.reshape(tokens, width), mine, 1, 0)
    cots = cascade(swap(pairs), top_token.reshape(1, 8, width // 8))
    cot = swap(cots).reshape(tokens, width).astype(jnp.float32)

    logit_diff = slope * jnp.sum(out_diff * cot, axis=-1)
    input_grad = (cot + logit_diff[:, None] * step).astype(jnp.bfloat16)
    logit_grad = logit_diff[:, None] * sign
    router_part = lax.dot_general(
        logit_grad[:, 1:], inputs, (((0,), (0,)), ((), ())), precision=HIGH
    )

    is_zero = (chosen == 0).astype(jnp.float32)
    zero_gate = gate * is_zero[:, 0] + (1.0 - gate) * is_zero[:, 1]
    routed = (is_zero[:, 0] + is_zero[:, 1]).reshape(micro, tok)
    earlier = jnp.tril(jnp.ones((tok, tok), jnp.float32), -1)
    slot_pos = jnp.sum(routed[:, None, :] * earlier, axis=-1).astype(jnp.int32)
    slot_ids = jnp.arange(capacity, dtype=jnp.int32)
    pick = ((slot_pos[:, None, :] == slot_ids[:, None]) & (routed[:, None, :] > 0.5)).astype(
        jnp.float32
    )
    scaled = (zero_gate[:, None] * cot).reshape(micro, tok, width)
    rows = jnp.einsum("mcu,mud->mcd", pick, scaled, precision=HIGH).astype(jnp.bfloat16)

    held = jnp.concatenate(
        [rows.reshape(micro * capacity, width).astype(jnp.float32), router_part], axis=0
    )
    half, power = to_half(held)
    powers = jnp.zeros((1, width), jnp.float16)
    powers = lax.dynamic_update_slice(powers, power[None].astype(jnp.float16), (0, 0))
    sent = jnp.concatenate([half, powers], axis=0)
    got = lax.all_gather(sent, "expert", axis=0, tiled=False)

    scale = jnp.exp2(got[:, -1, : micro * capacity + experts - 1].astype(jnp.float32))

    def received(first, size):
        part = got[:, first : first + size].astype(jnp.float32)
        return part * scale[:, first : first + size, None]

    others = jnp.sum(received(micro * capacity, experts - 1), axis=0)
    router_sum = jnp.concatenate([-jnp.sum(others, axis=0, keepdims=True), others], axis=0)
    router_grad = router_sum.T / (tokens * groups)

    weight = down_w[0]
    hidden_parts = []
    down_acc = 0.0
    for part in range(micro):
        slots = received(part * capacity, capacity).astype(jnp.bfloat16).reshape(-1, width)
        hidden_parts.append(
            lax.dot_general(
                weight, slots, (((1,), (1,)), ((), ())), preferred_element_type=jnp.float32
            ).astype(jnp.bfloat16)
        )
        down_acc = down_acc + lax.dot_general(
            hidden[0, part], slots, (((0,), (0,)), ((), ())), preferred_element_type=jnp.float32
        )
    hidden_grad = jnp.stack(hidden_parts).transpose(0, 2, 1)
    down_grad = down_acc
    return (
        input_grad.reshape(1, micro, tok, width),
        router_grad[None],
        hidden_grad[None],
        down_grad.astype(jnp.bfloat16)[None],
    )


def solution(mesh):
    placed = (
        P(None, "expert", None),
        P("section", None, "expert", None),
        P("section", None, "expert", None, None),
        P("section", None, None),
        P("section", None, "expert", None),
        P("section", None, None, "expert"),
        P("section", "expert", None),
    )
    return jax.shard_map(
        per_device,
        mesh=mesh,
        in_specs=placed,
        out_specs=(
            P("section", None, "expert", None),
            P("section", None, None),
            P("section", None, None, "expert"),
            P("section", "expert", None),
        ),
        check_vma=False,
    )
```

```python
import jax
import jax.numpy as jnp
from jax import lax
from jax.experimental import pallas as pl
from jax.experimental.pallas import tpu as pltpu
from jax.sharding import PartitionSpec as P

HIGH = lax.Precision.HIGHEST


def cascade_kernel(ur_ref, top_ref, out_ref):
    count = ur_ref.shape[0]
    cot = top_ref[0].astype(jnp.float32)
    for layer in reversed(range(count)):
        out_ref[layer] = cot.astype(jnp.bfloat16)
        if layer:
            prod = ur_ref[layer, 0].astype(jnp.float32) * cot
            total = prod[:, :128] + prod[:, 128:]
            for shift in (4, 2, 1):
                total = total + pltpu.roll(total, shift, 0)
            diff = jnp.sum(total, axis=1, keepdims=True)
            cot = cot + diff * ur_ref[layer, 1].astype(jnp.float32)
            cot = cot.astype(jnp.bfloat16).astype(jnp.float32)


def cascade(pairs, top_token):
    count = pairs.shape[0]
    vmem = pl.BlockSpec(memory_space=pltpu.VMEM)
    return pl.pallas_call(
        cascade_kernel,
        out_shape=jax.ShapeDtypeStruct((count, 8, 256), jnp.bfloat16),
        in_specs=[vmem, vmem],
        out_specs=vmem,
        compiler_params=pltpu.CompilerParams(vmem_limit_bytes=8 << 20),
        name="cascade",
    )(pairs, top_token)


def fetch_kernel(weight_ref, hidden_ref, _, weight_out, hidden_out, sems):
    copies = [
        pltpu.make_async_copy(weight_ref, weight_out, sems.at[0]),
        pltpu.make_async_copy(hidden_ref, hidden_out, sems.at[1]),
    ]
    for copy in copies:
        copy.start()
    for copy in copies:
        copy.wait()


def fetch(weight, hidden, after):
    vmem = pl.BlockSpec(memory_space=pltpu.VMEM)
    return pl.pallas_call(
        fetch_kernel,
        out_shape=(
            jax.ShapeDtypeStruct(weight.shape, weight.dtype),
            jax.ShapeDtypeStruct(hidden.shape, hidden.dtype),
        ),
        in_specs=[pl.BlockSpec(memory_space=pl.ANY)] * 3,
        out_specs=(vmem, vmem),
        scratch_shapes=[pltpu.SemaphoreType.DMA((2,))],
        compiler_params=pltpu.CompilerParams(vmem_limit_bytes=8 << 20),
        cost_estimate=pl.CostEstimate(flops=1 << 21, transcendentals=0, bytes_accessed=1 << 21),
        name="fetch",
    )(weight, hidden, after)


def in_pieces(value):
    high = value.astype(jnp.bfloat16)
    rest = value - high.astype(jnp.float32)
    middle = rest.astype(jnp.bfloat16)
    low = (rest - middle.astype(jnp.float32)).astype(jnp.bfloat16)
    return jnp.concatenate([high, middle, low], axis=0)


def dims(left, right):
    return (((left,), (right,)), ((), ()))


def prepare_kernel(
    ids_hbm, router_hbm, inputs_hbm, outs_hbm,
    pairs_ref, diff_ref,
    ids_ref, router_ref, inputs_ref, outs_ref, wide_ref, sems,
):
    copies = [
        pltpu.make_async_copy(far, near, sems.at[index])
        for index, (far, near) in enumerate(
            (
                (ids_hbm, ids_ref),
                (router_hbm, router_ref),
                (inputs_hbm, inputs_ref),
                (outs_hbm, outs_ref),
            )
        )
    ]
    for copy in copies:
        copy.start()
    for copy in copies:
        copy.wait()
    micro, _, tok = ids_ref.shape
    experts = router_ref.shape[0]
    pieces = in_pieces(router_ref[...])
    for part in range(micro):
        span = pl.ds(part * tok, tok)
        expert = lax.broadcasted_iota(jnp.int32, (experts, tok), 0)
        first, second = ids_ref[part, 0:1, :], ids_ref[part, 1:2, :]
        sign = (expert == first).astype(jnp.float32) - (expert == second).astype(jnp.float32)
        logits = lax.dot_general(
            pieces, inputs_ref[span, :], dims(1, 1), preferred_element_type=jnp.float32
        )
        logits = logits[:experts] + logits[experts : 2 * experts] + logits[2 * experts :]
        gate = jax.nn.sigmoid(jnp.sum(sign * logits, axis=0, keepdims=True))
        slope = in_pieces(gate * (1.0 - gate))
        spread = lax.dot_general(
            slope,
            jnp.ones((3, 128), jnp.bfloat16),
            dims(0, 0),
            preferred_element_type=jnp.float32,
        )
        sign = sign.astype(jnp.bfloat16)
        step = lax.dot_general(
            jnp.concatenate([sign, sign, sign], axis=0),
            pieces,
            dims(0, 0),
            preferred_element_type=jnp.float32,
        )
        diff = outs_ref[part, :, 0, :].astype(jnp.float32) - outs_ref[part, :, 1, :].astype(jnp.float32)
        diff_ref[span, :] = diff
        scaled = diff * spread[:, :1]
        chunk = wide_ref.shape[3]
        for row in range(8):
            columns = slice(row * chunk, (row + 1) * chunk)
            wide_ref[span, 0, row, :] = scaled[:, columns]
            wide_ref[span, 1, row, :] = step[:, columns]
    pairs_ref[...] = wide_ref[...].astype(jnp.bfloat16)


def prepare(chosen, router, inputs, outputs):
    tokens, width = inputs.shape
    pairs = (tokens, 2, 8, width // 8)
    return pl.pallas_call(
        prepare_kernel,
        out_shape=(
            jax.ShapeDtypeStruct(pairs, jnp.bfloat16),
            jax.ShapeDtypeStruct((tokens, width), jnp.float32),
        ),
        in_specs=[pl.BlockSpec(memory_space=pltpu.HBM)] * 4,
        scratch_shapes=[
            *(pltpu.VMEM(value.shape, value.dtype) for value in (chosen, router, inputs, outputs)),
            pltpu.VMEM(pairs, jnp.float32),
            pltpu.SemaphoreType.DMA((4,)),
        ],
        name="prepare",
    )(chosen, router, inputs, outputs)


def finish_kernel(
    slots_ref, weight_ref, hidden_ref, router_ref, grad_ref,
    hidden_out, down_out, router_out, grad_out,
    hidden_buf, down_buf, sems,
):
    copies = [
        pltpu.make_async_copy(router_ref, router_out, sems.at[0]),
        pltpu.make_async_copy(grad_ref, grad_out, sems.at[1]),
    ]
    for copy in copies:
        copy.start()
    micro = slots_ref.shape[0]
    width = weight_ref.shape[1]
    chunk = width // 4
    for index in range(4):
        span = pl.ds(index * chunk, chunk)
        total = 0.0
        for part in range(micro):
            total = total + lax.dot_general(
                hidden_ref[part], slots_ref[part, :, span], dims(1, 0),
                preferred_element_type=jnp.float32,
            )
        down_buf[:, span] = total.astype(jnp.bfloat16)
        copy = pltpu.make_async_copy(
            down_buf.at[:, span], down_out.at[:, span], sems.at[2 + index]
        )
        copy.start()
        copies.append(copy)
    for part in range(micro):
        hidden_buf[part] = lax.dot_general(
            weight_ref[...], slots_ref[part], dims(1, 1), preferred_element_type=jnp.float32
        ).astype(jnp.bfloat16)
        copy = pltpu.make_async_copy(
            hidden_buf.at[part], hidden_out.at[part], sems.at[6 + part]
        )
        copy.start()
        copies.append(copy)
    for copy in copies:
        copy.wait()


def finish(slots, weight, hidden, router_grad, input_grad):
    vmem = pl.BlockSpec(memory_space=pltpu.VMEM)
    anywhere = pl.BlockSpec(memory_space=pl.ANY)
    shapes = [
        jax.ShapeDtypeStruct(value.shape, value.dtype)
        for value in (hidden, weight, router_grad, input_grad)
    ]
    return pl.pallas_call(
        finish_kernel,
        out_shape=tuple(shapes),
        in_specs=[vmem] * 5,
        out_specs=tuple([anywhere] * 4),
        scratch_shapes=[
            pltpu.VMEM(hidden.shape, hidden.dtype),
            pltpu.VMEM(weight.shape, weight.dtype),
            pltpu.SemaphoreType.DMA((6 + hidden.shape[0],)),
        ],
        compiler_params=pltpu.CompilerParams(vmem_limit_bytes=16 << 20),
        name="finish",
    )(slots, weight, hidden, router_grad, input_grad)


def swap(value):
    return lax.all_to_all(value, "section", 0, 0, tiled=True)


def to_half(value):
    peak = jnp.max(jnp.abs(value), axis=-1, keepdims=True)
    power = jnp.clip(jnp.ceil(jnp.log2(jnp.maximum(peak, 1e-30))), -100.0, 120.0)
    return (value * jnp.exp2(-power)).astype(jnp.float16), power[..., 0]


def per_device(top_grad, layer_input, expert_out, router_w, expert_ids, hidden, down_w):
    micro, tok, width = top_grad.shape
    tokens = micro * tok
    sections = lax.axis_size("section")
    groups = lax.axis_size("expert")
    capacity = tok // 2
    inputs = layer_input[0].reshape(tokens, width).astype(jnp.float32)
    router = router_w[0]
    experts = router.shape[1]
    chosen = expert_ids[0].reshape(tokens, 2)

    logits = jnp.dot(inputs, router, precision=HIGH)
    select = (chosen[..., None] == jnp.arange(experts, dtype=jnp.int32)).astype(jnp.float32)
    sign = select[:, 0] - select[:, 1]
    gate = jax.nn.sigmoid(jnp.sum(sign * logits, axis=-1))
    slope = gate * (1.0 - gate)
    step = lax.dot_general(sign, router, (((1,), (1,)), ((), ())), precision=HIGH)

    pairs, out_diff = prepare(
        expert_ids[0].transpose(0, 2, 1),
        router.T,
        layer_input[0].reshape(tokens, width),
        expert_out[0],
    )
    mine = lax.axis_index("section")
    top_token = lax.dynamic_slice_in_dim(top_grad.reshape(tokens, width), mine, 1, 0)
    received_pairs = swap(pairs)
    cots = cascade(received_pairs, top_token.reshape(1, 8, width // 8))
    weight, saved_hidden = fetch(down_w[0], hidden[0].transpose(0, 2, 1), cots)
    cot = swap(cots).reshape(tokens, width).astype(jnp.float32)

    logit_diff = slope * jnp.sum(out_diff * cot, axis=-1)
    input_grad = (cot + logit_diff[:, None] * step).astype(jnp.bfloat16)
    logit_grad = logit_diff[:, None] * sign
    router_part = lax.dot_general(
        logit_grad[:, 1:], inputs, (((0,), (0,)), ((), ())), precision=HIGH
    )

    is_zero = (chosen == 0).astype(jnp.float32)
    zero_gate = gate * is_zero[:, 0] + (1.0 - gate) * is_zero[:, 1]
    routed = (is_zero[:, 0] + is_zero[:, 1]).reshape(micro, tok)
    earlier = jnp.tril(jnp.ones((tok, tok), jnp.float32), -1)
    slot_pos = jnp.sum(routed[:, None, :] * earlier, axis=-1).astype(jnp.int32)
    slot_ids = jnp.arange(capacity, dtype=jnp.int32)
    pick = ((slot_pos[:, None, :] == slot_ids[:, None]) & (routed[:, None, :] > 0.5)).astype(
        jnp.float32
    )
    scaled = (zero_gate[:, None] * cot).reshape(micro, tok, width)
    rows = jnp.einsum("mcu,mud->mcd", pick, scaled, precision=HIGH).astype(jnp.bfloat16)

    held = jnp.concatenate(
        [rows.reshape(micro * capacity, width).astype(jnp.float32), router_part], axis=0
    )
    half, power = to_half(held)
    powers = jnp.zeros((1, width), jnp.float16)
    powers = lax.dynamic_update_slice(powers, power[None].astype(jnp.float16), (0, 0))
    sent = jnp.concatenate([half, powers], axis=0)
    got = lax.all_gather(sent, "expert", axis=0, tiled=False)

    scale = jnp.exp2(got[:, -1, : micro * capacity + experts - 1].astype(jnp.float32))

    def received(first, size):
        part = got[:, first : first + size].astype(jnp.float32)
        return part * scale[:, first : first + size, None]

    others = jnp.sum(received(micro * capacity, experts - 1), axis=0)
    router_sum = jnp.concatenate([-jnp.sum(others, axis=0, keepdims=True), others], axis=0)
    slots = jnp.stack(
        [
            received(part * capacity, capacity).astype(jnp.bfloat16).reshape(-1, width)
            for part in range(micro)
        ]
    )
    hidden_grad, down_grad, router_grad, input_grad = finish(
        slots,
        weight,
        saved_hidden,
        router_sum / (tokens * groups),
        input_grad,
    )
    return (
        input_grad.reshape(1, micro, tok, width),
        router_grad.T[None],
        hidden_grad.transpose(0, 2, 1)[None],
        down_grad[None],
    )


def solution(mesh):
    placed = (
        P(None, "expert", None),
        P("section", None, "expert", None),
        P("section", None, "expert", None, None),
        P("section", None, None),
        P("section", None, "expert", None),
        P("section", None, None, "expert"),
        P("section", "expert", None),
    )
    return jax.shard_map(
        per_device,
        mesh=mesh,
        in_specs=placed,
        out_specs=(
            P("section", None, "expert", None),
            P("section", None, None),
            P("section", None, None, "expert"),
            P("section", "expert", None),
        ),
        check_vma=False,
    )
```

```python
import jax
import jax.numpy as jnp
from jax import lax
from jax.experimental import pallas as pl
from jax.experimental.pallas import tpu as pltpu
from jax.sharding import PartitionSpec as P

HIGH = lax.Precision.HIGHEST


BLOCK = 4


def spread_sum(prod):
    total = prod[:, :128] + prod[:, 128:]
    for shift in (4, 2, 1):
        total = total + pltpu.roll(total, shift, 0)
    return jnp.sum(total, axis=1, keepdims=True)


def cascade_kernel(ur_ref, top_ref, out_ref):
    count = ur_ref.shape[0]

    def scaled(layer):
        return ur_ref[layer, 0].astype(jnp.float32)

    def step(layer):
        return ur_ref[layer, 1].astype(jnp.float32)

    blocks = [
        list(range(first, max(first - BLOCK, -1), -1)) for first in range(count - 1, -1, -BLOCK)
    ]
    cross = {
        (low, high): spread_sum(scaled(low) * step(high))
        for block in blocks
        for high in block
        for low in block
        if 0 < low < high
    }
    cot = top_ref[0].astype(jnp.float32)
    for block in blocks:
        sums = {layer: spread_sum(scaled(layer) * cot) for layer in block if layer}
        for layer in block:
            out_ref[layer] = cot.astype(jnp.bfloat16)
            if layer:
                cot = cot + sums[layer] * step(layer)
                cot = cot.astype(jnp.bfloat16).astype(jnp.float32)
                for low in block:
                    if 0 < low < layer:
                        sums[low] = sums[low] + sums[layer] * cross[low, layer]


def cascade(pairs, top_token):
    count = pairs.shape[0]
    vmem = pl.BlockSpec(memory_space=pltpu.VMEM)
    return pl.pallas_call(
        cascade_kernel,
        out_shape=jax.ShapeDtypeStruct((count, 8, 256), jnp.bfloat16),
        in_specs=[vmem, vmem],
        out_specs=vmem,
        compiler_params=pltpu.CompilerParams(vmem_limit_bytes=8 << 20),
        name="cascade",
    )(pairs, top_token)


def fetch_kernel(weight_ref, hidden_ref, _, weight_out, hidden_out, sems):
    copies = [
        pltpu.make_async_copy(weight_ref, weight_out, sems.at[0]),
        pltpu.make_async_copy(hidden_ref, hidden_out, sems.at[1]),
    ]
    for copy in copies:
        copy.start()
    for copy in copies:
        copy.wait()


def fetch(weight, hidden, after):
    vmem = pl.BlockSpec(memory_space=pltpu.VMEM)
    return pl.pallas_call(
        fetch_kernel,
        out_shape=(
            jax.ShapeDtypeStruct(weight.shape, weight.dtype),
            jax.ShapeDtypeStruct(hidden.shape, hidden.dtype),
        ),
        in_specs=[pl.BlockSpec(memory_space=pl.ANY)] * 3,
        out_specs=(vmem, vmem),
        scratch_shapes=[pltpu.SemaphoreType.DMA((2,))],
        compiler_params=pltpu.CompilerParams(vmem_limit_bytes=8 << 20),
        cost_estimate=pl.CostEstimate(flops=1 << 21, transcendentals=0, bytes_accessed=1 << 21),
        name="fetch",
    )(weight, hidden, after)


def in_pieces(value):
    high = value.astype(jnp.bfloat16)
    rest = value - high.astype(jnp.float32)
    middle = rest.astype(jnp.bfloat16)
    low = (rest - middle.astype(jnp.float32)).astype(jnp.bfloat16)
    return jnp.concatenate([high, middle, low], axis=0)


def dims(left, right):
    return (((left,), (right,)), ((), ()))


def prepare_kernel(
    ids_hbm, router_hbm, inputs_hbm, outs_hbm,
    pairs_ref, diff_ref,
    ids_ref, router_ref, inputs_ref, outs_ref, wide_ref, sems,
):
    copies = [
        pltpu.make_async_copy(far, near, sems.at[index])
        for index, (far, near) in enumerate(
            (
                (ids_hbm, ids_ref),
                (router_hbm, router_ref),
                (inputs_hbm, inputs_ref),
                (outs_hbm, outs_ref),
            )
        )
    ]
    for copy in copies:
        copy.start()
    for copy in copies:
        copy.wait()
    micro, _, tok = ids_ref.shape
    experts = router_ref.shape[0]
    pieces = in_pieces(router_ref[...])
    for part in range(micro):
        span = pl.ds(part * tok, tok)
        expert = lax.broadcasted_iota(jnp.int32, (experts, tok), 0)
        first, second = ids_ref[part, 0:1, :], ids_ref[part, 1:2, :]
        sign = (expert == first).astype(jnp.float32) - (expert == second).astype(jnp.float32)
        logits = lax.dot_general(
            pieces, inputs_ref[span, :], dims(1, 1), preferred_element_type=jnp.float32
        )
        logits = logits[:experts] + logits[experts : 2 * experts] + logits[2 * experts :]
        gate = jax.nn.sigmoid(jnp.sum(sign * logits, axis=0, keepdims=True))
        slope = in_pieces(gate * (1.0 - gate))
        spread = lax.dot_general(
            slope,
            jnp.ones((3, 128), jnp.bfloat16),
            dims(0, 0),
            preferred_element_type=jnp.float32,
        )
        sign = sign.astype(jnp.bfloat16)
        step = lax.dot_general(
            jnp.concatenate([sign, sign, sign], axis=0),
            pieces,
            dims(0, 0),
            preferred_element_type=jnp.float32,
        )
        diff = outs_ref[part, :, 0, :].astype(jnp.float32) - outs_ref[part, :, 1, :].astype(jnp.float32)
        diff_ref[span, :] = diff
        scaled = diff * spread[:, :1]
        chunk = wide_ref.shape[3]
        for row in range(8):
            columns = slice(row * chunk, (row + 1) * chunk)
            wide_ref[span, 0, row, :] = scaled[:, columns]
            wide_ref[span, 1, row, :] = step[:, columns]
    pairs_ref[...] = wide_ref[...].astype(jnp.bfloat16)


def prepare(chosen, router, inputs, outputs):
    tokens, width = inputs.shape
    pairs = (tokens, 2, 8, width // 8)
    return pl.pallas_call(
        prepare_kernel,
        out_shape=(
            jax.ShapeDtypeStruct(pairs, jnp.bfloat16),
            jax.ShapeDtypeStruct((tokens, width), jnp.float32),
        ),
        in_specs=[pl.BlockSpec(memory_space=pltpu.HBM)] * 4,
        scratch_shapes=[
            *(pltpu.VMEM(value.shape, value.dtype) for value in (chosen, router, inputs, outputs)),
            pltpu.VMEM(pairs, jnp.float32),
            pltpu.SemaphoreType.DMA((4,)),
        ],
        name="prepare",
    )(chosen, router, inputs, outputs)


def finish_kernel(
    slots_ref, weight_ref, hidden_ref, router_ref, grad_ref,
    hidden_out, down_out, router_out, grad_out,
    hidden_buf, down_buf, sems,
):
    copies = [
        pltpu.make_async_copy(router_ref, router_out, sems.at[0]),
        pltpu.make_async_copy(grad_ref, grad_out, sems.at[1]),
    ]
    for copy in copies:
        copy.start()
    micro = hidden_ref.shape[0]
    width = weight_ref.shape[1]
    capacity = slots_ref.shape[1] // micro

    def slots(part, span):
        value = slots_ref[:, part * capacity : (part + 1) * capacity, span]
        return value.reshape(-1, value.shape[-1])

    chunk = width // 4
    for index in range(4):
        span = slice(index * chunk, (index + 1) * chunk)
        total = 0.0
        for part in range(micro):
            total = total + lax.dot_general(
                hidden_ref[part], slots(part, span), dims(1, 0),
                preferred_element_type=jnp.float32,
            )
        down_buf[:, span] = total.astype(jnp.bfloat16)
        copy = pltpu.make_async_copy(
            down_buf.at[:, span], down_out.at[:, span], sems.at[2 + index]
        )
        copy.start()
        copies.append(copy)
    for part in range(micro):
        hidden_buf[part] = lax.dot_general(
            weight_ref[...], slots(part, slice(None)), dims(1, 1),
            preferred_element_type=jnp.float32,
        ).astype(jnp.bfloat16)
        copy = pltpu.make_async_copy(
            hidden_buf.at[part], hidden_out.at[part], sems.at[6 + part]
        )
        copy.start()
        copies.append(copy)
    for copy in copies:
        copy.wait()


def finish(slots, weight, hidden, router_grad, input_grad):
    vmem = pl.BlockSpec(memory_space=pltpu.VMEM)
    anywhere = pl.BlockSpec(memory_space=pl.ANY)
    shapes = [
        jax.ShapeDtypeStruct(value.shape, value.dtype)
        for value in (hidden, weight, router_grad, input_grad)
    ]
    return pl.pallas_call(
        finish_kernel,
        out_shape=tuple(shapes),
        in_specs=[vmem] * 5,
        out_specs=tuple([anywhere] * 4),
        scratch_shapes=[
            pltpu.VMEM(hidden.shape, hidden.dtype),
            pltpu.VMEM(weight.shape, weight.dtype),
            pltpu.SemaphoreType.DMA((6 + hidden.shape[0],)),
        ],
        compiler_params=pltpu.CompilerParams(vmem_limit_bytes=16 << 20),
        name="finish",
    )(slots, weight, hidden, router_grad, input_grad)


def swap(value):
    return lax.all_to_all(value, "section", 0, 0, tiled=True)


def to_half(value):
    peak = jnp.max(jnp.abs(value), axis=-1, keepdims=True)
    power = jnp.clip(jnp.ceil(jnp.log2(jnp.maximum(peak, 1e-30))), -100.0, 120.0)
    return (value * jnp.exp2(-power)).astype(jnp.float16), power[..., 0]


def per_device(top_grad, layer_input, expert_out, router_w, expert_ids, hidden, down_w):
    micro, tok, width = top_grad.shape
    tokens = micro * tok
    sections = lax.axis_size("section")
    groups = lax.axis_size("expert")
    capacity = tok // 2
    inputs = layer_input[0].reshape(tokens, width).astype(jnp.float32)
    router = router_w[0]
    experts = router.shape[1]
    chosen = expert_ids[0].reshape(tokens, 2)

    logits = jnp.dot(inputs, router, precision=HIGH)
    select = (chosen[..., None] == jnp.arange(experts, dtype=jnp.int32)).astype(jnp.float32)
    sign = select[:, 0] - select[:, 1]
    gate = jax.nn.sigmoid(jnp.sum(sign * logits, axis=-1))
    slope = gate * (1.0 - gate)
    step = lax.dot_general(sign, router, (((1,), (1,)), ((), ())), precision=HIGH)

    pairs, out_diff = prepare(
        expert_ids[0].transpose(0, 2, 1),
        router.T,
        layer_input[0].reshape(tokens, width),
        expert_out[0],
    )
    mine = lax.axis_index("section")
    top_token = lax.dynamic_slice_in_dim(top_grad.reshape(tokens, width), mine, 1, 0)
    received_pairs = swap(pairs)
    cots = cascade(received_pairs, top_token.reshape(1, 8, width // 8))
    weight, saved_hidden = fetch(down_w[0], hidden[0].transpose(0, 2, 1), cots)
    cot = swap(cots).reshape(tokens, width).astype(jnp.float32)

    logit_diff = slope * jnp.sum(out_diff * cot, axis=-1)
    input_grad = (cot + logit_diff[:, None] * step).astype(jnp.bfloat16)
    logit_grad = logit_diff[:, None] * sign
    router_part = lax.dot_general(
        logit_grad[:, 1:], inputs, (((0,), (0,)), ((), ())), precision=HIGH
    )

    is_zero = (chosen == 0).astype(jnp.float32)
    zero_gate = gate * is_zero[:, 0] + (1.0 - gate) * is_zero[:, 1]
    routed = (is_zero[:, 0] + is_zero[:, 1]).reshape(micro, tok)
    earlier = jnp.tril(jnp.ones((tok, tok), jnp.float32), -1)
    slot_pos = jnp.sum(routed[:, None, :] * earlier, axis=-1).astype(jnp.int32)
    slot_ids = jnp.arange(capacity, dtype=jnp.int32)
    pick = ((slot_pos[:, None, :] == slot_ids[:, None]) & (routed[:, None, :] > 0.5)).astype(
        jnp.float32
    )
    scaled = (zero_gate[:, None] * cot).reshape(micro, tok, width)
    rows = jnp.einsum("mcu,mud->mcd", pick, scaled, precision=HIGH).astype(jnp.bfloat16)

    held = jnp.concatenate(
        [rows.reshape(micro * capacity, width).astype(jnp.float32), router_part], axis=0
    )
    half, power = to_half(held)
    powers = jnp.zeros((1, width), jnp.float16)
    powers = lax.dynamic_update_slice(powers, power[None].astype(jnp.float16), (0, 0))
    sent = jnp.concatenate([half, powers], axis=0)
    got = lax.all_gather(sent, "expert", axis=0, tiled=False)

    scale = jnp.exp2(got[:, -1, : micro * capacity + experts - 1].astype(jnp.float32))

    def received(first, size):
        part = got[:, first : first + size].astype(jnp.float32)
        return part * scale[:, first : first + size, None]

    others = jnp.sum(received(micro * capacity, experts - 1), axis=0)
    router_sum = jnp.concatenate([-jnp.sum(others, axis=0, keepdims=True), others], axis=0)
    slots = received(0, micro * capacity).astype(jnp.bfloat16)
    hidden_grad, down_grad, router_grad, input_grad = finish(
        slots,
        weight,
        saved_hidden,
        router_sum / (tokens * groups),
        input_grad,
    )
    return (
        input_grad.reshape(1, micro, tok, width),
        router_grad.T[None],
        hidden_grad.transpose(0, 2, 1)[None],
        down_grad[None],
    )


def solution(mesh):
    placed = (
        P(None, "expert", None),
        P("section", None, "expert", None),
        P("section", None, "expert", None, None),
        P("section", None, None),
        P("section", None, "expert", None),
        P("section", None, None, "expert"),
        P("section", "expert", None),
    )
    return jax.shard_map(
        per_device,
        mesh=mesh,
        in_specs=placed,
        out_specs=(
            P("section", None, "expert", None),
            P("section", None, None),
            P("section", None, None, "expert"),
            P("section", "expert", None),
        ),
        check_vma=False,
    )
```

```python
import jax
import jax.numpy as jnp
from jax import lax
from jax.experimental import pallas as pl
from jax.experimental.pallas import tpu as pltpu
from jax.sharding import PartitionSpec as P

HIGH = lax.Precision.HIGHEST


BLOCK = 4


def spread_sum(prod):
    total = prod[:, :128] + prod[:, 128:]
    for shift in (4, 2, 1):
        total = total + pltpu.roll(total, shift, 0)
    return jnp.sum(total, axis=1, keepdims=True)


def cascade_kernel(ur_ref, top_ref, out_ref):
    count = ur_ref.shape[0]

    def scaled(layer):
        return ur_ref[layer, 0].astype(jnp.float32)

    def step(layer):
        return ur_ref[layer, 1].astype(jnp.float32)

    blocks = [
        list(range(first, max(first - BLOCK, -1), -1)) for first in range(count - 1, -1, -BLOCK)
    ]
    cross = {
        (low, high): spread_sum(scaled(low) * step(high))
        for block in blocks
        for high in block
        for low in block
        if 0 < low < high
    }
    cot = top_ref[0].astype(jnp.float32)
    for block in blocks:
        sums = {layer: spread_sum(scaled(layer) * cot) for layer in block if layer}
        for layer in block:
            out_ref[layer] = cot.astype(jnp.bfloat16)
            if layer:
                cot = cot + sums[layer] * step(layer)
                cot = cot.astype(jnp.bfloat16).astype(jnp.float32)
                for low in block:
                    if 0 < low < layer:
                        sums[low] = sums[low] + sums[layer] * cross[low, layer]


def cascade(pairs, top_token):
    count = pairs.shape[0]
    vmem = pl.BlockSpec(memory_space=pltpu.VMEM)
    return pl.pallas_call(
        cascade_kernel,
        out_shape=jax.ShapeDtypeStruct((count, 8, 256), jnp.bfloat16),
        in_specs=[vmem, vmem],
        out_specs=vmem,
        compiler_params=pltpu.CompilerParams(vmem_limit_bytes=8 << 20),
        name="cascade",
    )(pairs, top_token)


def fetch_kernel(weight_ref, hidden_ref, _, weight_out, hidden_out, sems):
    copies = [
        pltpu.make_async_copy(weight_ref, weight_out, sems.at[0]),
        pltpu.make_async_copy(hidden_ref, hidden_out, sems.at[1]),
    ]
    for copy in copies:
        copy.start()
    for copy in copies:
        copy.wait()


def fetch(weight, hidden, after):
    vmem = pl.BlockSpec(memory_space=pltpu.VMEM)
    return pl.pallas_call(
        fetch_kernel,
        out_shape=(
            jax.ShapeDtypeStruct(weight.shape, weight.dtype),
            jax.ShapeDtypeStruct(hidden.shape, hidden.dtype),
        ),
        in_specs=[pl.BlockSpec(memory_space=pl.ANY)] * 3,
        out_specs=(vmem, vmem),
        scratch_shapes=[pltpu.SemaphoreType.DMA((2,))],
        compiler_params=pltpu.CompilerParams(vmem_limit_bytes=8 << 20),
        cost_estimate=pl.CostEstimate(flops=1 << 21, transcendentals=0, bytes_accessed=1 << 21),
        name="fetch",
    )(weight, hidden, after)


def in_pieces(value, axis=0):
    high = value.astype(jnp.bfloat16)
    rest = value - high.astype(jnp.float32)
    middle = rest.astype(jnp.bfloat16)
    low = (rest - middle.astype(jnp.float32)).astype(jnp.bfloat16)
    return jnp.concatenate([high, middle, low], axis=axis)


def dims(left, right):
    return (((left,), (right,)), ((), ()))


def prepare_kernel(
    ids_hbm, router_hbm, inputs_hbm, outs_hbm,
    pairs_hbm,
    ids_ref, router_ref, inputs_ref, outs_ref, wide_ref, pairs_ref, sems,
):
    copies = [
        pltpu.make_async_copy(far, near, sems.at[index])
        for index, (far, near) in enumerate(
            (
                (ids_hbm, ids_ref),
                (router_hbm, router_ref),
                (inputs_hbm, inputs_ref),
                (outs_hbm, outs_ref),
            )
        )
    ]
    for copy in copies:
        copy.start()
    for copy in copies:
        copy.wait()
    sent = []
    micro, _, tok = ids_ref.shape
    experts = router_ref.shape[0]
    pieces = in_pieces(router_ref[...])
    for part in range(micro):
        span = pl.ds(part * tok, tok)
        expert = lax.broadcasted_iota(jnp.int32, (experts, tok), 0)
        first, second = ids_ref[part, 0:1, :], ids_ref[part, 1:2, :]
        sign = (expert == first).astype(jnp.float32) - (expert == second).astype(jnp.float32)
        logits = lax.dot_general(
            pieces, inputs_ref[span, :], dims(1, 1), preferred_element_type=jnp.float32
        )
        logits = logits[:experts] + logits[experts : 2 * experts] + logits[2 * experts :]
        gate = jax.nn.sigmoid(jnp.sum(sign * logits, axis=0, keepdims=True))
        slope = in_pieces(gate * (1.0 - gate))
        spread = lax.dot_general(
            slope,
            jnp.ones((3, 128), jnp.bfloat16),
            dims(0, 0),
            preferred_element_type=jnp.float32,
        )
        sign = sign.astype(jnp.bfloat16)
        step = lax.dot_general(
            jnp.concatenate([sign, sign, sign], axis=0),
            pieces,
            dims(0, 0),
            preferred_element_type=jnp.float32,
        )
        diff = outs_ref[part, :, 0, :].astype(jnp.float32) - outs_ref[part, :, 1, :].astype(jnp.float32)
        scaled = diff * spread[:, :1]
        chunk = wide_ref.shape[3]
        for row in range(8):
            columns = slice(row * chunk, (row + 1) * chunk)
            wide_ref[span, 0, row, :] = scaled[:, columns]
            wide_ref[span, 1, row, :] = step[:, columns]
        pairs_ref[span] = wide_ref[span].astype(jnp.bfloat16)
        copy = pltpu.make_async_copy(pairs_ref.at[span], pairs_hbm.at[span], sems.at[4 + part])
        copy.start()
        sent.append(copy)
    for copy in sent:
        copy.wait()


def prepare(chosen, router, inputs, outputs):
    tokens, width = inputs.shape
    pairs = (tokens, 2, 8, width // 8)
    return pl.pallas_call(
        prepare_kernel,
        out_shape=jax.ShapeDtypeStruct(pairs, jnp.bfloat16),
        in_specs=[pl.BlockSpec(memory_space=pltpu.HBM)] * 4,
        out_specs=pl.BlockSpec(memory_space=pltpu.HBM),
        scratch_shapes=[
            *(pltpu.VMEM(value.shape, value.dtype) for value in (chosen, router, inputs, outputs)),
            pltpu.VMEM(pairs, jnp.float32),
            pltpu.VMEM(pairs, jnp.bfloat16),
            pltpu.SemaphoreType.DMA((4 + chosen.shape[0],)),
        ],
        name="prepare",
    )(chosen, router, inputs, outputs)


def middle_kernel(
    cots_ref, outs_ref, inputs_ref, step_ref, sign_ref, slope_ref, pick_ref,
    held_ref, grad_ref,
    wide_ref,
):
    micro, tok = outs_ref.shape[:2]
    capacity, experts = pick_ref.shape[1], sign_ref.shape[1]
    count = micro * capacity
    wide_ref[...] = cots_ref[...].astype(jnp.float32)
    groups, router = [], 0.0
    for part in range(micro):
        span = pl.ds(part * tok, tok)
        cot = jnp.concatenate([wide_ref[span, row, :] for row in range(8)], axis=1)
        diff = outs_ref[part, :, 0, :].astype(jnp.float32) - outs_ref[part, :, 1, :].astype(jnp.float32)
        change = slope_ref[span, :] * jnp.sum(diff * cot, axis=1, keepdims=True)
        grad_ref[span, :] = (cot + change * step_ref[span, :]).astype(jnp.bfloat16)
        rows = lax.dot_general(
            in_pieces(pick_ref[part]), cot.astype(jnp.bfloat16), dims(1, 0),
            preferred_element_type=jnp.float32,
        )
        rows = rows[:capacity] + rows[capacity : 2 * capacity] + rows[2 * capacity :]
        groups.append(rows.astype(jnp.bfloat16).astype(jnp.float32))
        parts = lax.dot_general(
            in_pieces(change * sign_ref[span, :], 1), inputs_ref[span, :], dims(0, 0),
            preferred_element_type=jnp.float32,
        )
        router = router + (parts[:experts] + parts[experts : 2 * experts] + parts[2 * experts :])
    groups.append(router)
    lane = lax.broadcasted_iota(jnp.int32, (capacity, 128), 1)
    row = lax.broadcasted_iota(jnp.int32, (capacity, 128), 0)
    powers = jnp.zeros((1, 128), jnp.float32)
    for index, value in enumerate(groups):
        peak = jnp.max(jnp.abs(value), axis=1, keepdims=True)
        power = jnp.clip(jnp.ceil(jnp.log2(jnp.maximum(peak, 1e-30))), -100.0, 120.0)
        held_ref[index * capacity : (index + 1) * capacity, :] = value * jnp.exp2(-power)
        powers = powers + jnp.sum(
            jnp.where(lane == row + index * capacity, power, 0.0), axis=0, keepdims=True
        )
    held_ref[count : count + 1, :] = jnp.zeros((1, held_ref.shape[1]), jnp.float32)
    held_ref[count : count + 1, :128] = powers


def middle(cots, outputs, inputs, step, sign, slope, pick):
    vmem = pl.BlockSpec(memory_space=pltpu.VMEM)
    rows = pick.shape[0] * pick.shape[1] + sign.shape[1]
    return pl.pallas_call(
        middle_kernel,
        out_shape=(
            jax.ShapeDtypeStruct((rows, inputs.shape[1]), jnp.float32),
            jax.ShapeDtypeStruct(inputs.shape, jnp.bfloat16),
        ),
        in_specs=[vmem] * 7,
        out_specs=(vmem, vmem),
        scratch_shapes=[pltpu.VMEM(cots.shape, jnp.float32)],
        compiler_params=pltpu.CompilerParams(vmem_limit_bytes=8 << 20),
        name="middle",
    )(cots, outputs, inputs, step, sign, slope, pick)


def finish_kernel(
    slots_ref, weight_ref, hidden_ref, router_ref, grad_ref,
    hidden_out, down_out, router_out, grad_out,
    hidden_buf, down_buf, sems,
):
    copies = [
        pltpu.make_async_copy(router_ref, router_out, sems.at[0]),
        pltpu.make_async_copy(grad_ref, grad_out, sems.at[1]),
    ]
    for copy in copies:
        copy.start()
    micro = hidden_ref.shape[0]
    width = weight_ref.shape[1]
    capacity = slots_ref.shape[1] // micro

    def slots(part, span):
        value = slots_ref[:, part * capacity : (part + 1) * capacity, span]
        return value.reshape(-1, value.shape[-1])

    chunk = width // 4
    for index in range(4):
        span = slice(index * chunk, (index + 1) * chunk)
        total = 0.0
        for part in range(micro):
            total = total + lax.dot_general(
                hidden_ref[part], slots(part, span), dims(1, 0),
                preferred_element_type=jnp.float32,
            )
        down_buf[:, span] = total.astype(jnp.bfloat16)
        copy = pltpu.make_async_copy(
            down_buf.at[:, span], down_out.at[:, span], sems.at[2 + index]
        )
        copy.start()
        copies.append(copy)
    for part in range(micro):
        hidden_buf[part] = lax.dot_general(
            weight_ref[...], slots(part, slice(None)), dims(1, 1),
            preferred_element_type=jnp.float32,
        ).astype(jnp.bfloat16)
        copy = pltpu.make_async_copy(
            hidden_buf.at[part], hidden_out.at[part], sems.at[6 + part]
        )
        copy.start()
        copies.append(copy)
    for copy in copies:
        copy.wait()


def finish(slots, weight, hidden, router_grad, input_grad):
    vmem = pl.BlockSpec(memory_space=pltpu.VMEM)
    anywhere = pl.BlockSpec(memory_space=pl.ANY)
    shapes = [
        jax.ShapeDtypeStruct(value.shape, value.dtype)
        for value in (hidden, weight, router_grad, input_grad)
    ]
    return pl.pallas_call(
        finish_kernel,
        out_shape=tuple(shapes),
        in_specs=[vmem] * 5,
        out_specs=tuple([anywhere] * 4),
        scratch_shapes=[
            pltpu.VMEM(hidden.shape, hidden.dtype),
            pltpu.VMEM(weight.shape, weight.dtype),
            pltpu.SemaphoreType.DMA((6 + hidden.shape[0],)),
        ],
        compiler_params=pltpu.CompilerParams(vmem_limit_bytes=16 << 20),
        name="finish",
    )(slots, weight, hidden, router_grad, input_grad)


def swap(value):
    return lax.all_to_all(value, "section", 0, 0, tiled=True)


def per_device(top_grad, layer_input, expert_out, router_w, expert_ids, hidden, down_w):
    micro, tok, width = top_grad.shape
    tokens = micro * tok
    sections = lax.axis_size("section")
    groups = lax.axis_size("expert")
    capacity = tok // 2
    inputs = layer_input[0].reshape(tokens, width).astype(jnp.float32)
    router = router_w[0]
    experts = router.shape[1]
    chosen = expert_ids[0].reshape(tokens, 2)

    logits = jnp.dot(inputs, router, precision=HIGH)
    select = (chosen[..., None] == jnp.arange(experts, dtype=jnp.int32)).astype(jnp.float32)
    sign = select[:, 0] - select[:, 1]
    gate = jax.nn.sigmoid(jnp.sum(sign * logits, axis=-1))
    slope = gate * (1.0 - gate)
    step = lax.dot_general(sign, router, (((1,), (1,)), ((), ())), precision=HIGH)

    pairs = prepare(
        expert_ids[0].transpose(0, 2, 1),
        router.T,
        layer_input[0].reshape(tokens, width),
        expert_out[0],
    )
    mine = lax.axis_index("section")
    top_token = lax.dynamic_slice_in_dim(top_grad.reshape(tokens, width), mine, 1, 0)
    received_pairs = swap(pairs)
    cots = cascade(received_pairs, top_token.reshape(1, 8, width // 8))
    weight, saved_hidden = fetch(down_w[0], hidden[0].transpose(0, 2, 1), cots)
    is_zero = (chosen == 0).astype(jnp.float32)
    zero_gate = gate * is_zero[:, 0] + (1.0 - gate) * is_zero[:, 1]
    routed = (is_zero[:, 0] + is_zero[:, 1]).reshape(micro, tok)
    earlier = jnp.tril(jnp.ones((tok, tok), jnp.float32), -1)
    slot_pos = jnp.sum(routed[:, None, :] * earlier, axis=-1).astype(jnp.int32)
    slot_ids = jnp.arange(capacity, dtype=jnp.int32)
    pick = ((slot_pos[:, None, :] == slot_ids[:, None]) & (routed[:, None, :] > 0.5)).astype(
        jnp.float32
    )
    held, input_grad = middle(
        swap(cots),
        expert_out[0],
        layer_input[0].reshape(tokens, width),
        step,
        sign,
        slope[:, None],
        pick * zero_gate.reshape(micro, 1, tok),
    )
    got = lax.all_gather(held.astype(jnp.float16), "expert", axis=0, tiled=False)
    count = micro * capacity
    scale = jnp.exp2(got[:, count, : count + experts].astype(jnp.float32))

    def received(first, size):
        part = got[:, first : first + size].astype(jnp.float32)
        return part * scale[:, first : first + size, None]

    others = jnp.sum(received(count + 1, experts - 1), axis=0)
    router_sum = jnp.concatenate([-jnp.sum(others, axis=0, keepdims=True), others], axis=0)
    slots = received(0, count).astype(jnp.bfloat16)
    hidden_grad, down_grad, router_grad, input_grad = finish(
        slots,
        weight,
        saved_hidden,
        router_sum / (tokens * groups),
        input_grad,
    )
    return (
        input_grad.reshape(1, micro, tok, width),
        router_grad.T[None],
        hidden_grad.transpose(0, 2, 1)[None],
        down_grad[None],
    )


def solution(mesh):
    placed = (
        P(None, "expert", None),
        P("section", None, "expert", None),
        P("section", None, "expert", None, None),
        P("section", None, None),
        P("section", None, "expert", None),
        P("section", None, None, "expert"),
        P("section", "expert", None),
    )
    return jax.shard_map(
        per_device,
        mesh=mesh,
        in_specs=placed,
        out_specs=(
            P("section", None, "expert", None),
            P("section", None, None),
            P("section", None, None, "expert"),
            P("section", "expert", None),
        ),
        check_vma=False,
    )
```

```python
import jax
import jax.numpy as jnp
from jax import lax
from jax.experimental import pallas as pl
from jax.experimental.pallas import tpu as pltpu
from jax.sharding import PartitionSpec as P

HIGH = lax.Precision.HIGHEST


BLOCK = 4


def spread_sum(prod):
    total = prod[:, :128] + prod[:, 128:]
    for shift in (4, 2, 1):
        total = total + pltpu.roll(total, shift, 0)
    return jnp.sum(total, axis=1, keepdims=True)


def cascade_kernel(ur_ref, top_ref, _pick, _slope, _step, _weight, out_ref):
    count = ur_ref.shape[0]

    def scaled(layer):
        return ur_ref[layer, 0].astype(jnp.float32)

    def step(layer):
        return ur_ref[layer, 1].astype(jnp.float32)

    blocks = [
        list(range(first, max(first - BLOCK, -1), -1)) for first in range(count - 1, -1, -BLOCK)
    ]
    cross = {
        (low, high): spread_sum(scaled(low) * step(high))
        for block in blocks
        for high in block
        for low in block
        if 0 < low < high
    }
    cot = top_ref[0].astype(jnp.float32)
    for block in blocks:
        sums = {layer: spread_sum(scaled(layer) * cot) for layer in block if layer}
        for layer in block:
            out_ref[layer] = cot.astype(jnp.bfloat16)
            if layer:
                cot = cot + sums[layer] * step(layer)
                cot = cot.astype(jnp.bfloat16).astype(jnp.float32)
                for low in block:
                    if 0 < low < layer:
                        sums[low] = sums[low] + sums[layer] * cross[low, layer]


def cascade(pairs, top_token, before):
    count = pairs.shape[0]
    vmem = pl.BlockSpec(memory_space=pltpu.VMEM)
    return pl.pallas_call(
        cascade_kernel,
        out_shape=jax.ShapeDtypeStruct((count, 8, 256), jnp.bfloat16),
        in_specs=[vmem] * 6,
        out_specs=vmem,
        compiler_params=pltpu.CompilerParams(vmem_limit_bytes=8 << 20),
        name="cascade",
    )(pairs, top_token, *before)


def fetch_kernel(weight_ref, hidden_ref, weight_out, hidden_out, sems):
    copies = [
        pltpu.make_async_copy(weight_ref, weight_out, sems.at[0]),
        pltpu.make_async_copy(hidden_ref, hidden_out, sems.at[1]),
    ]
    for copy in copies:
        copy.start()
    for copy in copies:
        copy.wait()


def fetch(weight, hidden):
    vmem = pl.BlockSpec(memory_space=pltpu.VMEM)
    return pl.pallas_call(
        fetch_kernel,
        out_shape=(
            jax.ShapeDtypeStruct(weight.shape, weight.dtype),
            jax.ShapeDtypeStruct(hidden.shape, hidden.dtype),
        ),
        in_specs=[pl.BlockSpec(memory_space=pl.ANY)] * 2,
        out_specs=(vmem, vmem),
        scratch_shapes=[pltpu.SemaphoreType.DMA((2,))],
        compiler_params=pltpu.CompilerParams(vmem_limit_bytes=8 << 20),
        cost_estimate=pl.CostEstimate(flops=1 << 21, transcendentals=0, bytes_accessed=1 << 21),
        name="fetch",
    )(weight, hidden)


def in_pieces(value, axis=0):
    high = value.astype(jnp.bfloat16)
    rest = value - high.astype(jnp.float32)
    middle = rest.astype(jnp.bfloat16)
    low = (rest - middle.astype(jnp.float32)).astype(jnp.bfloat16)
    return jnp.concatenate([high, middle, low], axis=axis)


def dims(left, right):
    return (((left,), (right,)), ((), ()))


def prepare_kernel(
    ids_hbm, router_hbm, inputs_hbm, outs_hbm,
    pairs_hbm,
    ids_ref, router_ref, inputs_ref, outs_ref, wide_ref, pairs_ref, sems,
):
    copies = [
        pltpu.make_async_copy(far, near, sems.at[index])
        for index, (far, near) in enumerate(
            (
                (ids_hbm, ids_ref),
                (router_hbm, router_ref),
                (inputs_hbm, inputs_ref),
                (outs_hbm, outs_ref),
            )
        )
    ]
    for copy in copies:
        copy.start()
    for copy in copies:
        copy.wait()
    sent = []
    micro, _, tok = ids_ref.shape
    experts = router_ref.shape[0]
    pieces = in_pieces(router_ref[...])
    for part in range(micro):
        span = pl.ds(part * tok, tok)
        expert = lax.broadcasted_iota(jnp.int32, (experts, tok), 0)
        first, second = ids_ref[part, 0:1, :], ids_ref[part, 1:2, :]
        sign = (expert == first).astype(jnp.float32) - (expert == second).astype(jnp.float32)
        logits = lax.dot_general(
            pieces, inputs_ref[span, :], dims(1, 1), preferred_element_type=jnp.float32
        )
        logits = logits[:experts] + logits[experts : 2 * experts] + logits[2 * experts :]
        gate = jax.nn.sigmoid(jnp.sum(sign * logits, axis=0, keepdims=True))
        slope = in_pieces(gate * (1.0 - gate))
        spread = lax.dot_general(
            slope,
            jnp.ones((3, 128), jnp.bfloat16),
            dims(0, 0),
            preferred_element_type=jnp.float32,
        )
        sign = sign.astype(jnp.bfloat16)
        step = lax.dot_general(
            jnp.concatenate([sign, sign, sign], axis=0),
            pieces,
            dims(0, 0),
            preferred_element_type=jnp.float32,
        )
        diff = outs_ref[part, :, 0, :].astype(jnp.float32) - outs_ref[part, :, 1, :].astype(jnp.float32)
        scaled = diff * spread[:, :1]
        chunk = wide_ref.shape[3]
        for row in range(8):
            columns = slice(row * chunk, (row + 1) * chunk)
            wide_ref[span, 0, row, :] = scaled[:, columns]
            wide_ref[span, 1, row, :] = step[:, columns]
        pairs_ref[span] = wide_ref[span].astype(jnp.bfloat16)
        copy = pltpu.make_async_copy(pairs_ref.at[span], pairs_hbm.at[span], sems.at[4 + part])
        copy.start()
        sent.append(copy)
    for copy in sent:
        copy.wait()


def prepare(chosen, router, inputs, outputs):
    tokens, width = inputs.shape
    pairs = (tokens, 2, 8, width // 8)
    return pl.pallas_call(
        prepare_kernel,
        out_shape=jax.ShapeDtypeStruct(pairs, jnp.bfloat16),
        in_specs=[pl.BlockSpec(memory_space=pltpu.HBM)] * 4,
        out_specs=pl.BlockSpec(memory_space=pltpu.HBM),
        scratch_shapes=[
            *(pltpu.VMEM(value.shape, value.dtype) for value in (chosen, router, inputs, outputs)),
            pltpu.VMEM(pairs, jnp.float32),
            pltpu.VMEM(pairs, jnp.bfloat16),
            pltpu.SemaphoreType.DMA((4 + chosen.shape[0],)),
        ],
        name="prepare",
    )(chosen, router, inputs, outputs)


def middle_kernel(
    cots_ref, outs_ref, inputs_ref, step_ref, sign_ref, slope_ref, pick_ref,
    held_ref, grad_ref,
    wide_ref,
):
    micro, tok = outs_ref.shape[:2]
    capacity, experts = pick_ref.shape[1], sign_ref.shape[1]
    count = micro * capacity
    wide_ref[...] = cots_ref[...].astype(jnp.float32)
    groups, router = [], 0.0
    for part in range(micro):
        span = pl.ds(part * tok, tok)
        cot = jnp.concatenate([wide_ref[span, row, :] for row in range(8)], axis=1)
        diff = outs_ref[part, :, 0, :].astype(jnp.float32) - outs_ref[part, :, 1, :].astype(jnp.float32)
        change = slope_ref[span, :] * jnp.sum(diff * cot, axis=1, keepdims=True)
        grad_ref[span, :] = (cot + change * step_ref[span, :]).astype(jnp.bfloat16)
        rows = lax.dot_general(
            in_pieces(pick_ref[part]), cot.astype(jnp.bfloat16), dims(1, 0),
            preferred_element_type=jnp.float32,
        )
        rows = rows[:capacity] + rows[capacity : 2 * capacity] + rows[2 * capacity :]
        groups.append(rows.astype(jnp.bfloat16).astype(jnp.float32))
        parts = lax.dot_general(
            in_pieces(change * sign_ref[span, :], 1), inputs_ref[span, :], dims(0, 0),
            preferred_element_type=jnp.float32,
        )
        router = router + (parts[:experts] + parts[experts : 2 * experts] + parts[2 * experts :])
    groups.append(router)
    lane = lax.broadcasted_iota(jnp.int32, (capacity, 128), 1)
    row = lax.broadcasted_iota(jnp.int32, (capacity, 128), 0)
    powers = jnp.zeros((1, 128), jnp.float32)
    for index, value in enumerate(groups):
        peak = jnp.max(jnp.abs(value), axis=1, keepdims=True)
        power = jnp.clip(jnp.ceil(jnp.log2(jnp.maximum(peak, 1e-30))), -100.0, 120.0)
        held_ref[index * capacity : (index + 1) * capacity, :] = value * jnp.exp2(-power)
        powers = powers + jnp.sum(
            jnp.where(lane == row + index * capacity, power, 0.0), axis=0, keepdims=True
        )
    held_ref[count : count + 1, :] = jnp.zeros((1, held_ref.shape[1]), jnp.float32)
    held_ref[count : count + 1, :128] = powers


def middle(cots, outputs, inputs, step, sign, slope, pick):
    vmem = pl.BlockSpec(memory_space=pltpu.VMEM)
    rows = pick.shape[0] * pick.shape[1] + sign.shape[1]
    return pl.pallas_call(
        middle_kernel,
        out_shape=(
            jax.ShapeDtypeStruct((rows, inputs.shape[1]), jnp.float32),
            jax.ShapeDtypeStruct(inputs.shape, jnp.bfloat16),
        ),
        in_specs=[vmem] * 7,
        out_specs=(vmem, vmem),
        scratch_shapes=[pltpu.VMEM(cots.shape, jnp.float32)],
        compiler_params=pltpu.CompilerParams(vmem_limit_bytes=8 << 20),
        name="middle",
    )(cots, outputs, inputs, step, sign, slope, pick)


def finish_kernel(
    slots_ref, weight_ref, hidden_ref, router_ref, grad_ref,
    hidden_out, down_out, router_out, grad_out,
    hidden_buf, down_buf, sems,
):
    copies = [
        pltpu.make_async_copy(router_ref, router_out, sems.at[0]),
        pltpu.make_async_copy(grad_ref, grad_out, sems.at[1]),
    ]
    for copy in copies:
        copy.start()
    micro = hidden_ref.shape[0]
    width = weight_ref.shape[1]
    capacity = slots_ref.shape[1] // micro

    def slots(part, span):
        value = slots_ref[:, part * capacity : (part + 1) * capacity, span]
        return value.reshape(-1, value.shape[-1])

    chunk = width // 4
    for index in range(4):
        span = slice(index * chunk, (index + 1) * chunk)
        total = 0.0
        for part in range(micro):
            total = total + lax.dot_general(
                hidden_ref[part], slots(part, span), dims(1, 0),
                preferred_element_type=jnp.float32,
            )
        down_buf[:, span] = total.astype(jnp.bfloat16)
        copy = pltpu.make_async_copy(
            down_buf.at[:, span], down_out.at[:, span], sems.at[2 + index]
        )
        copy.start()
        copies.append(copy)
    for part in range(micro):
        hidden_buf[part] = lax.dot_general(
            weight_ref[...], slots(part, slice(None)), dims(1, 1),
            preferred_element_type=jnp.float32,
        ).astype(jnp.bfloat16)
        copy = pltpu.make_async_copy(
            hidden_buf.at[part], hidden_out.at[part], sems.at[6 + part]
        )
        copy.start()
        copies.append(copy)
    for copy in copies:
        copy.wait()


def finish(slots, weight, hidden, router_grad, input_grad):
    vmem = pl.BlockSpec(memory_space=pltpu.VMEM)
    anywhere = pl.BlockSpec(memory_space=pl.ANY)
    shapes = [
        jax.ShapeDtypeStruct(value.shape, value.dtype)
        for value in (hidden, weight, router_grad, input_grad)
    ]
    return pl.pallas_call(
        finish_kernel,
        out_shape=tuple(shapes),
        in_specs=[vmem] * 5,
        out_specs=tuple([anywhere] * 4),
        scratch_shapes=[
            pltpu.VMEM(hidden.shape, hidden.dtype),
            pltpu.VMEM(weight.shape, weight.dtype),
            pltpu.SemaphoreType.DMA((6 + hidden.shape[0],)),
        ],
        compiler_params=pltpu.CompilerParams(vmem_limit_bytes=16 << 20),
        name="finish",
    )(slots, weight, hidden, router_grad, input_grad)


def swap(value):
    return lax.all_to_all(value, "section", 0, 0, tiled=True)


def per_device(top_grad, layer_input, expert_out, router_w, expert_ids, hidden, down_w):
    micro, tok, width = top_grad.shape
    tokens = micro * tok
    sections = lax.axis_size("section")
    groups = lax.axis_size("expert")
    capacity = tok // 2
    inputs = layer_input[0].reshape(tokens, width).astype(jnp.float32)
    router = router_w[0]
    experts = router.shape[1]
    chosen = expert_ids[0].reshape(tokens, 2)

    logits = jnp.dot(inputs, router, precision=HIGH)
    select = (chosen[..., None] == jnp.arange(experts, dtype=jnp.int32)).astype(jnp.float32)
    sign = select[:, 0] - select[:, 1]
    gate = jax.nn.sigmoid(jnp.sum(sign * logits, axis=-1))
    slope = gate * (1.0 - gate)
    step = lax.dot_general(sign, router, (((1,), (1,)), ((), ())), precision=HIGH)

    pairs = prepare(
        expert_ids[0].transpose(0, 2, 1),
        router.T,
        layer_input[0].reshape(tokens, width),
        expert_out[0],
    )
    mine = lax.axis_index("section")
    top_token = lax.dynamic_slice_in_dim(top_grad.reshape(tokens, width), mine, 1, 0)
    received_pairs = swap(pairs)
    weight, saved_hidden = fetch(down_w[0], hidden[0].transpose(0, 2, 1))
    is_zero = (chosen == 0).astype(jnp.float32)
    zero_gate = gate * is_zero[:, 0] + (1.0 - gate) * is_zero[:, 1]
    routed = (is_zero[:, 0] + is_zero[:, 1]).reshape(micro, tok)
    earlier = jnp.tril(jnp.ones((tok, tok), jnp.float32), -1)
    slot_pos = jnp.sum(routed[:, None, :] * earlier, axis=-1).astype(jnp.int32)
    slot_ids = jnp.arange(capacity, dtype=jnp.int32)
    pick = ((slot_pos[:, None, :] == slot_ids[:, None]) & (routed[:, None, :] > 0.5)).astype(
        jnp.float32
    )
    pick = pick * zero_gate.reshape(micro, 1, tok)
    before = (pick, slope[:, None], step, weight)
    cots = cascade(received_pairs, top_token.reshape(1, 8, width // 8), before)
    held, input_grad = middle(
        swap(cots),
        expert_out[0],
        layer_input[0].reshape(tokens, width),
        step,
        sign,
        before[1],
        pick,
    )
    got = lax.all_gather(held.astype(jnp.float16), "expert", axis=0, tiled=False)
    count = micro * capacity
    scale = jnp.exp2(got[:, count, : count + experts].astype(jnp.float32))

    def received(first, size):
        part = got[:, first : first + size].astype(jnp.float32)
        return part * scale[:, first : first + size, None]

    others = jnp.sum(received(count + 1, experts - 1), axis=0)
    router_sum = jnp.concatenate([-jnp.sum(others, axis=0, keepdims=True), others], axis=0)
    slots = received(0, count).astype(jnp.bfloat16)
    hidden_grad, down_grad, router_grad, input_grad = finish(
        slots,
        weight,
        saved_hidden,
        router_sum / (tokens * groups),
        input_grad,
    )
    return (
        input_grad.reshape(1, micro, tok, width),
        router_grad.T[None],
        hidden_grad.transpose(0, 2, 1)[None],
        down_grad[None],
    )


def solution(mesh):
    placed = (
        P(None, "expert", None),
        P("section", None, "expert", None),
        P("section", None, "expert", None, None),
        P("section", None, None),
        P("section", None, "expert", None),
        P("section", None, None, "expert"),
        P("section", "expert", None),
    )
    return jax.shard_map(
        per_device,
        mesh=mesh,
        in_specs=placed,
        out_specs=(
            P("section", None, "expert", None),
            P("section", None, None),
            P("section", None, None, "expert"),
            P("section", "expert", None),
        ),
        check_vma=False,
    )
```

```python
import jax
import jax.numpy as jnp
from jax import lax
from jax.experimental import pallas as pl
from jax.experimental.pallas import tpu as pltpu
from jax.sharding import PartitionSpec as P

HIGH = lax.Precision.HIGHEST


BLOCK = 8


def spread_sum(prod):
    total = prod[:, :128] + prod[:, 128:]
    for shift in (4, 2, 1):
        total = total + pltpu.roll(total, shift, 0)
    return jnp.sum(total, axis=1, keepdims=True)


def cascade_kernel(ur_ref, top_ref, out_ref):
    count = ur_ref.shape[0]

    def scaled(layer):
        return ur_ref[layer, 0].astype(jnp.float32)

    def step(layer):
        return ur_ref[layer, 1].astype(jnp.float32)

    blocks = [
        list(range(first, max(first - BLOCK, -1), -1)) for first in range(count - 1, -1, -BLOCK)
    ]
    cross = {
        (low, high): spread_sum(scaled(low) * step(high))
        for block in blocks
        for high in block
        for low in block
        if 0 < low < high
    }
    cot = top_ref[0].astype(jnp.float32)
    for block in blocks:
        sums = {layer: spread_sum(scaled(layer) * cot) for layer in block if layer}
        for layer in block:
            out_ref[layer] = cot.astype(jnp.bfloat16)
            if layer:
                cot = cot + sums[layer] * step(layer)
                cot = cot.astype(jnp.bfloat16).astype(jnp.float32)
                for low in block:
                    if 0 < low < layer:
                        sums[low] = sums[low] + sums[layer] * cross[low, layer]


def cascade(pairs, top_token):
    count = pairs.shape[0]
    vmem = pl.BlockSpec(memory_space=pltpu.VMEM)
    return pl.pallas_call(
        cascade_kernel,
        out_shape=jax.ShapeDtypeStruct((count, 8, 256), jnp.bfloat16),
        in_specs=[vmem, vmem],
        out_specs=vmem,
        compiler_params=pltpu.CompilerParams(vmem_limit_bytes=8 << 20),
        name="cascade",
    )(pairs, top_token)


def fetch_kernel(weight_ref, hidden_ref, _, weight_out, hidden_out, sems):
    copies = [
        pltpu.make_async_copy(weight_ref, weight_out, sems.at[0]),
        pltpu.make_async_copy(hidden_ref, hidden_out, sems.at[1]),
    ]
    for copy in copies:
        copy.start()
    for copy in copies:
        copy.wait()


def fetch(weight, hidden, after):
    vmem = pl.BlockSpec(memory_space=pltpu.VMEM)
    return pl.pallas_call(
        fetch_kernel,
        out_shape=(
            jax.ShapeDtypeStruct(weight.shape, weight.dtype),
            jax.ShapeDtypeStruct(hidden.shape, hidden.dtype),
        ),
        in_specs=[pl.BlockSpec(memory_space=pl.ANY)] * 3,
        out_specs=(vmem, vmem),
        scratch_shapes=[pltpu.SemaphoreType.DMA((2,))],
        compiler_params=pltpu.CompilerParams(vmem_limit_bytes=8 << 20),
        cost_estimate=pl.CostEstimate(flops=1 << 21, transcendentals=0, bytes_accessed=1 << 21),
        name="fetch",
    )(weight, hidden, after)


def in_pieces(value, axis=0):
    high = value.astype(jnp.bfloat16)
    rest = value - high.astype(jnp.float32)
    middle = rest.astype(jnp.bfloat16)
    low = (rest - middle.astype(jnp.float32)).astype(jnp.bfloat16)
    return jnp.concatenate([high, middle, low], axis=axis)


def dims(left, right):
    return (((left,), (right,)), ((), ()))


def prepare_kernel(
    ids_hbm, router_hbm, inputs_hbm, outs_hbm,
    pairs_hbm,
    ids_ref, router_ref, inputs_ref, outs_ref, wide_ref, pairs_ref, sems,
):
    copies = [
        pltpu.make_async_copy(far, near, sems.at[index])
        for index, (far, near) in enumerate(
            (
                (ids_hbm, ids_ref),
                (router_hbm, router_ref),
                (inputs_hbm, inputs_ref),
                (outs_hbm, outs_ref),
            )
        )
    ]
    for copy in copies:
        copy.start()
    for copy in copies[:2]:
        copy.wait()
    sent, spreads = [], []
    micro, _, tok = ids_ref.shape
    experts = router_ref.shape[0]
    pieces = in_pieces(router_ref[...])
    chunk = wide_ref.shape[3]
    copies[2].wait()
    for part in range(micro):
        span = pl.ds(part * tok, tok)
        expert = lax.broadcasted_iota(jnp.int32, (experts, tok), 0)
        first, second = ids_ref[part, 0:1, :], ids_ref[part, 1:2, :]
        sign = (expert == first).astype(jnp.float32) - (expert == second).astype(jnp.float32)
        logits = lax.dot_general(
            pieces, inputs_ref[span, :], dims(1, 1), preferred_element_type=jnp.float32
        )
        logits = logits[:experts] + logits[experts : 2 * experts] + logits[2 * experts :]
        gate = jax.nn.sigmoid(jnp.sum(sign * logits, axis=0, keepdims=True))
        slope = in_pieces(gate * (1.0 - gate))
        spread = lax.dot_general(
            slope,
            jnp.ones((3, 128), jnp.bfloat16),
            dims(0, 0),
            preferred_element_type=jnp.float32,
        )
        sign = sign.astype(jnp.bfloat16)
        step = lax.dot_general(
            jnp.concatenate([sign, sign, sign], axis=0),
            pieces,
            dims(0, 0),
            preferred_element_type=jnp.float32,
        )
        spreads.append(spread[:, :1])
        for row in range(8):
            wide_ref[span, 1, row, :] = step[:, row * chunk : (row + 1) * chunk]
    copies[3].wait()
    for part in range(micro):
        span = pl.ds(part * tok, tok)
        diff = outs_ref[part, :, 0, :].astype(jnp.float32) - outs_ref[part, :, 1, :].astype(jnp.float32)
        scaled = diff * spreads[part]
        for row in range(8):
            wide_ref[span, 0, row, :] = scaled[:, row * chunk : (row + 1) * chunk]
        pairs_ref[span] = wide_ref[span].astype(jnp.bfloat16)
        copy = pltpu.make_async_copy(pairs_ref.at[span], pairs_hbm.at[span], sems.at[4 + part])
        copy.start()
        sent.append(copy)
    for copy in sent:
        copy.wait()


def prepare(chosen, router, inputs, outputs):
    tokens, width = inputs.shape
    pairs = (tokens, 2, 8, width // 8)
    return pl.pallas_call(
        prepare_kernel,
        out_shape=jax.ShapeDtypeStruct(pairs, jnp.bfloat16),
        in_specs=[pl.BlockSpec(memory_space=pltpu.HBM)] * 4,
        out_specs=pl.BlockSpec(memory_space=pltpu.HBM),
        scratch_shapes=[
            *(pltpu.VMEM(value.shape, value.dtype) for value in (chosen, router, inputs, outputs)),
            pltpu.VMEM(pairs, jnp.float32),
            pltpu.VMEM(pairs, jnp.bfloat16),
            pltpu.SemaphoreType.DMA((4 + chosen.shape[0],)),
        ],
        name="prepare",
    )(chosen, router, inputs, outputs)


def middle_kernel(
    cots_ref, outs_ref, inputs_ref, step_ref, sign_ref, slope_ref, pick_ref,
    held_ref, grad_ref,
    wide_ref,
):
    micro, tok = outs_ref.shape[:2]
    capacity, experts = pick_ref.shape[1], sign_ref.shape[1]
    count = micro * capacity
    wide_ref[...] = cots_ref[...].astype(jnp.float32)
    groups, router = [], 0.0
    for part in range(micro):
        span = pl.ds(part * tok, tok)
        cot = jnp.concatenate([wide_ref[span, row, :] for row in range(8)], axis=1)
        diff = outs_ref[part, :, 0, :].astype(jnp.float32) - outs_ref[part, :, 1, :].astype(jnp.float32)
        change = slope_ref[span, :] * jnp.sum(diff * cot, axis=1, keepdims=True)
        grad_ref[span, :] = (cot + change * step_ref[span, :]).astype(jnp.bfloat16)
        rows = lax.dot_general(
            in_pieces(pick_ref[part]), cot.astype(jnp.bfloat16), dims(1, 0),
            preferred_element_type=jnp.float32,
        )
        rows = rows[:capacity] + rows[capacity : 2 * capacity] + rows[2 * capacity :]
        groups.append(rows.astype(jnp.bfloat16).astype(jnp.float32))
        parts = lax.dot_general(
            in_pieces(change * sign_ref[span, :], 1), inputs_ref[span, :], dims(0, 0),
            preferred_element_type=jnp.float32,
        )
        router = router + (parts[:experts] + parts[experts : 2 * experts] + parts[2 * experts :])
    groups.append(router)
    lane = lax.broadcasted_iota(jnp.int32, (capacity, 128), 1)
    row = lax.broadcasted_iota(jnp.int32, (capacity, 128), 0)
    powers = jnp.zeros((1, 128), jnp.float32)
    for index, value in enumerate(groups):
        peak = jnp.max(jnp.abs(value), axis=1, keepdims=True)
        power = jnp.clip(jnp.ceil(jnp.log2(jnp.maximum(peak, 1e-30))), -100.0, 120.0)
        held_ref[index * capacity : (index + 1) * capacity, :] = value * jnp.exp2(-power)
        powers = powers + jnp.sum(
            jnp.where(lane == row + index * capacity, power, 0.0), axis=0, keepdims=True
        )
    held_ref[count : count + 1, :] = jnp.zeros((1, held_ref.shape[1]), jnp.float32)
    held_ref[count : count + 1, :128] = powers


def middle(cots, outputs, inputs, step, sign, slope, pick):
    vmem = pl.BlockSpec(memory_space=pltpu.VMEM)
    rows = pick.shape[0] * pick.shape[1] + sign.shape[1]
    return pl.pallas_call(
        middle_kernel,
        out_shape=(
            jax.ShapeDtypeStruct((rows, inputs.shape[1]), jnp.float32),
            jax.ShapeDtypeStruct(inputs.shape, jnp.bfloat16),
        ),
        in_specs=[vmem] * 7,
        out_specs=(vmem, vmem),
        scratch_shapes=[pltpu.VMEM(cots.shape, jnp.float32)],
        compiler_params=pltpu.CompilerParams(vmem_limit_bytes=8 << 20),
        name="middle",
    )(cots, outputs, inputs, step, sign, slope, pick)


def finish_kernel(
    slots_ref, weight_ref, hidden_ref, router_ref, grad_ref,
    hidden_out, down_out, router_out, grad_out,
    hidden_buf, down_buf, sems,
):
    copies = [
        pltpu.make_async_copy(router_ref, router_out, sems.at[0]),
        pltpu.make_async_copy(grad_ref, grad_out, sems.at[1]),
    ]
    for copy in copies:
        copy.start()
    micro = hidden_ref.shape[0]
    width = weight_ref.shape[1]
    capacity = slots_ref.shape[1] // micro

    def slots(part, span):
        value = slots_ref[:, part * capacity : (part + 1) * capacity, span]
        return value.reshape(-1, value.shape[-1])

    chunk = width // 4
    for index in range(4):
        span = slice(index * chunk, (index + 1) * chunk)
        total = 0.0
        for part in range(micro):
            total = total + lax.dot_general(
                hidden_ref[part], slots(part, span), dims(1, 0),
                preferred_element_type=jnp.float32,
            )
        down_buf[:, span] = total.astype(jnp.bfloat16)
        copy = pltpu.make_async_copy(
            down_buf.at[:, span], down_out.at[:, span], sems.at[2 + index]
        )
        copy.start()
        copies.append(copy)
    for part in range(micro):
        hidden_buf[part] = lax.dot_general(
            weight_ref[...], slots(part, slice(None)), dims(1, 1),
            preferred_element_type=jnp.float32,
        ).astype(jnp.bfloat16)
        copy = pltpu.make_async_copy(
            hidden_buf.at[part], hidden_out.at[part], sems.at[6 + part]
        )
        copy.start()
        copies.append(copy)
    for copy in copies:
        copy.wait()


def finish(slots, weight, hidden, router_grad, input_grad):
    vmem = pl.BlockSpec(memory_space=pltpu.VMEM)
    anywhere = pl.BlockSpec(memory_space=pl.ANY)
    shapes = [
        jax.ShapeDtypeStruct(value.shape, value.dtype)
        for value in (hidden, weight, router_grad, input_grad)
    ]
    return pl.pallas_call(
        finish_kernel,
        out_shape=tuple(shapes),
        in_specs=[vmem] * 5,
        out_specs=tuple([anywhere] * 4),
        scratch_shapes=[
            pltpu.VMEM(hidden.shape, hidden.dtype),
            pltpu.VMEM(weight.shape, weight.dtype),
            pltpu.SemaphoreType.DMA((6 + hidden.shape[0],)),
        ],
        compiler_params=pltpu.CompilerParams(vmem_limit_bytes=16 << 20),
        name="finish",
    )(slots, weight, hidden, router_grad, input_grad)


def swap(value):
    return lax.all_to_all(value, "section", 0, 0, tiled=True)


def per_device(top_grad, layer_input, expert_out, router_w, expert_ids, hidden, down_w):
    micro, tok, width = top_grad.shape
    tokens = micro * tok
    sections = lax.axis_size("section")
    groups = lax.axis_size("expert")
    capacity = tok // 2
    inputs = layer_input[0].reshape(tokens, width).astype(jnp.float32)
    router = router_w[0]
    experts = router.shape[1]
    chosen = expert_ids[0].reshape(tokens, 2)

    logits = jnp.dot(inputs, router, precision=HIGH)
    select = (chosen[..., None] == jnp.arange(experts, dtype=jnp.int32)).astype(jnp.float32)
    sign = select[:, 0] - select[:, 1]
    gate = jax.nn.sigmoid(jnp.sum(sign * logits, axis=-1))
    slope = gate * (1.0 - gate)
    step = lax.dot_general(sign, router, (((1,), (1,)), ((), ())), precision=HIGH)

    pairs = prepare(
        expert_ids[0].transpose(0, 2, 1),
        router.T,
        layer_input[0].reshape(tokens, width),
        expert_out[0],
    )
    mine = lax.axis_index("section")
    top_token = lax.dynamic_slice_in_dim(top_grad.reshape(tokens, width), mine, 1, 0)
    received_pairs = swap(pairs)
    cots = cascade(received_pairs, top_token.reshape(1, 8, width // 8))
    weight, saved_hidden = fetch(down_w[0], hidden[0].transpose(0, 2, 1), cots)
    is_zero = (chosen == 0).astype(jnp.float32)
    zero_gate = gate * is_zero[:, 0] + (1.0 - gate) * is_zero[:, 1]
    routed = (is_zero[:, 0] + is_zero[:, 1]).reshape(micro, tok)
    earlier = jnp.tril(jnp.ones((tok, tok), jnp.float32), -1)
    slot_pos = jnp.sum(routed[:, None, :] * earlier, axis=-1).astype(jnp.int32)
    slot_ids = jnp.arange(capacity, dtype=jnp.int32)
    pick = ((slot_pos[:, None, :] == slot_ids[:, None]) & (routed[:, None, :] > 0.5)).astype(
        jnp.float32
    )
    held, input_grad = middle(
        swap(cots),
        expert_out[0],
        layer_input[0].reshape(tokens, width),
        step,
        sign,
        slope[:, None],
        pick * zero_gate.reshape(micro, 1, tok),
    )
    got = lax.all_gather(held.astype(jnp.float16), "expert", axis=0, tiled=False)
    count = micro * capacity
    scale = jnp.exp2(got[:, count, : count + experts].astype(jnp.float32))

    def received(first, size):
        part = got[:, first : first + size].astype(jnp.float32)
        return part * scale[:, first : first + size, None]

    others = jnp.sum(received(count + 1, experts - 1), axis=0)
    router_sum = jnp.concatenate([-jnp.sum(others, axis=0, keepdims=True), others], axis=0)
    slots = received(0, count).astype(jnp.bfloat16)
    hidden_grad, down_grad, router_grad, input_grad = finish(
        slots,
        weight,
        saved_hidden,
        router_sum / (tokens * groups),
        input_grad,
    )
    return (
        input_grad.reshape(1, micro, tok, width),
        router_grad.T[None],
        hidden_grad.transpose(0, 2, 1)[None],
        down_grad[None],
    )


def solution(mesh):
    placed = (
        P(None, "expert", None),
        P("section", None, "expert", None),
        P("section", None, "expert", None, None),
        P("section", None, None),
        P("section", None, "expert", None),
        P("section", None, None, "expert"),
        P("section", "expert", None),
    )
    return jax.shard_map(
        per_device,
        mesh=mesh,
        in_specs=placed,
        out_specs=(
            P("section", None, "expert", None),
            P("section", None, None),
            P("section", None, None, "expert"),
            P("section", "expert", None),
        ),
        check_vma=False,
    )
```
